8 devices in a mesh: dp: 1 (over z), sp: 2 (over y), cp: 4 (over x, core).
Axes of the slice: x: 2, y: 2, z: 1, core: 2. Of those that a mesh axis runs over, the one named last changes fastest.
Arguments:
- hidden: bfloat16 [8, 2048, 4096], P('dp', ('cp', 'sp'))
- w_qkv: bfloat16 [4096, 3, 32, 128], replicated
- w_out: bfloat16 [32, 128, 4096], replicated
- norm_gain: bfloat16 [4096], replicated
- w_up: bfloat16 [4096, 16384], replicated
- b_up: bfloat16 [16384], replicated
- w_down: bfloat16 [16384, 4096], replicated
- b_down: bfloat16 [4096], replicated
Outputs:
- output: bfloat16 [8, 2048, 4096], P('dp', ('cp', 'sp'))
All inputs are finite; a program needn't handle non-finite values.
Results may differ from the reference program's by a relative error of at most 0.0103326.
Values are sent between devices in bfloat16 or wider.
A program may use at most 1.75 GiB of HBM per device.

```python
import math
import jax
import jax.numpy as jnp
from jax import lax

BATCH_SIZE = 8
SEQ_LEN = 2048
MODEL_DIM = 4096
NUM_HEADS = 32
HEAD_DIM = 128
MLP_DIM = 16384
Q_BLOCK = min(SEQ_LEN, 512)
NORM_EPS = 1e-6


def setup_inputs(seed: int = 0, part: int = 0) -> dict:
    key_list = jax.random.split(jax.random.key(seed), 8)
    act_key = jax.random.fold_in(key_list[0], part)
    qk_gain = (0.5 * math.log(SEQ_LEN)) ** 0.25
    out_gain = 0.8 * SEQ_LEN ** 0.25
    proj_gain = jnp.array([qk_gain, qk_gain, 1.0], jnp.float32).reshape(1, 3, 1, 1) * MODEL_DIM ** -0.5
    hidden = jax.random.normal(act_key, (BATCH_SIZE, SEQ_LEN, MODEL_DIM), jnp.float32)
    w_qkv = jax.random.normal(key_list[1], (MODEL_DIM, 3, NUM_HEADS, HEAD_DIM), jnp.float32) * proj_gain
    w_out = jax.random.normal(key_list[2], (NUM_HEADS, HEAD_DIM, MODEL_DIM), jnp.float32) * (out_gain * (NUM_HEADS * HEAD_DIM) ** -0.5)
    norm_gain = 1.0 + 0.3 * jax.random.normal(key_list[3], (MODEL_DIM,), jnp.float32)
    w_up = jax.random.normal(key_list[4], (MODEL_DIM, MLP_DIM), jnp.float32) * MODEL_DIM ** -0.5
    b_up = 0.5 * jax.random.normal(key_list[5], (MLP_DIM,), jnp.float32)
    w_down = jax.random.normal(key_list[6], (MLP_DIM, MODEL_DIM), jnp.float32) * MLP_DIM ** -0.5
    b_down = 0.5 * jax.random.normal(key_list[7], (MODEL_DIM,), jnp.float32)
    return dict(hidden=hidden.astype(jnp.bfloat16), w_qkv=w_qkv.astype(jnp.bfloat16), w_out=w_out.astype(jnp.bfloat16), norm_gain=norm_gain.astype(jnp.bfloat16), w_up=w_up.astype(jnp.bfloat16), b_up=b_up.astype(jnp.bfloat16), w_down=w_down.astype(jnp.bfloat16), b_down=b_down.astype(jnp.bfloat16))


def attend_head(head_args):
    q_head, k_head, v_head = head_args
    v_wide = v_head.astype(jnp.float32)
    q_blocks = q_head.reshape(SEQ_LEN // Q_BLOCK, Q_BLOCK, HEAD_DIM)

    def attend_rows(q_rows):
        scores = jnp.dot(q_rows, k_head.T, preferred_element_type=jnp.float32) * (HEAD_DIM ** -0.5)
        exp_scores = jnp.exp(scores - jnp.max(scores, axis=-1, keepdims=True))
        return jnp.dot(exp_scores, v_wide) / jnp.sum(exp_scores, axis=-1, keepdims=True)

    return lax.map(attend_rows, q_blocks).reshape(SEQ_LEN, HEAD_DIM)


def reference(hidden, w_qkv, w_out, norm_gain, w_up, b_up, w_down, b_down):
    qkv_proj = jnp.einsum("btc,cjhd->jbhtd", hidden.astype(jnp.float32), w_qkv.astype(jnp.float32)).astype(jnp.bfloat16)
    heads_flat = qkv_proj.reshape(3, BATCH_SIZE * NUM_HEADS, SEQ_LEN, HEAD_DIM)
    attn_heads = lax.map(attend_head, (heads_flat[0], heads_flat[1], heads_flat[2]))
    attn_heads = attn_heads.astype(jnp.bfloat16).reshape(BATCH_SIZE, NUM_HEADS, SEQ_LEN, HEAD_DIM)
    attn_out = jnp.einsum("bhtd,hdc->btc", attn_heads.astype(jnp.float32), w_out.astype(jnp.float32)).astype(jnp.bfloat16)
    residual = (hidden.astype(jnp.float32) + attn_out.astype(jnp.float32)).astype(jnp.bfloat16)
    resid_wide = residual.astype(jnp.float32)
    inv_rms = lax.rsqrt(jnp.mean(resid_wide * resid_wide, axis=-1, keepdims=True) + NORM_EPS)
    normed = (resid_wide * inv_rms * norm_gain.astype(jnp.float32)).astype(jnp.bfloat16)
    up_proj = jnp.einsum("btc,cf->btf", normed.astype(jnp.float32), w_up.astype(jnp.float32)) + b_up.astype(jnp.float32)
    up_act = jax.nn.gelu(up_proj, approximate=True).astype(jnp.bfloat16)
    down_proj = jnp.einsum("btf,fc->btc", up_act.astype(jnp.float32), w_down.astype(jnp.float32)) + b_down.astype(jnp.float32)
    return (resid_wide + down_proj).astype(jnp.bfloat16)
```

```python
import functools
import math

import jax
import jax.numpy as jnp
from jax import lax
from jax.experimental import pallas as pl
from jax.experimental.pallas import tpu as pltpu
from jax.sharding import PartitionSpec as P

NORM_EPS = 1e-6
VMEM_BYTES = 63 * 2**20
BF = jnp.bfloat16
F32 = jnp.float32
ANY = pl.BlockSpec(memory_space=pl.ANY)

ORDER = (0, 2, 4, 1, 6, 3, 5, 7)
PIECES = 8


def peer(rel):
    i, j = lax.axis_index("cp"), lax.axis_index("sp")
    kx, kc, ky = rel // 4, (rel // 2) % 2, rel % 2
    x = lax.rem(i // 2 + kx, 2)
    core = lax.rem(lax.rem(i, 2) + kc, 2)
    cp, sp = x * 2 + core, lax.rem(j + ky, 2)
    return {"cp": cp, "sp": sp}, cp * 2 + sp


def greet():
    bar = pltpu.get_barrier_semaphore()
    for rel in range(1, PIECES):
        pl.semaphore_signal(bar, inc=1, device_id=peer(rel)[0], device_id_type=pl.DeviceIdType.MESH)
    pl.semaphore_wait(bar, PIECES - 1)


def params(**kw):
    return pltpu.CompilerParams(vmem_limit_bytes=VMEM_BYTES, **kw)


def qkv_kernel(hid, w_ref, o_ref, row_out, xs, own_sem, send_sem, recv_sem, out_sem, *, n_tiles, kp):
    t = pl.program_id(0)
    chunk = t // n_tiles

    def send(slot):
        dev, row = peer(ORDER[slot])
        return pltpu.make_async_remote_copy(
            src_ref=hid.at[row], dst_ref=xs.at[slot], send_sem=send_sem.at[slot - 1], recv_sem=recv_sem.at[slot - 1],
            device_id=dev, device_id_type=pl.DeviceIdType.MESH)

    def keep(slot):
        return pltpu.make_async_copy(xs.at[slot], row_out.at[slot], out_sem.at[slot])

    @pl.when(t == 0)
    def _():
        own = pltpu.make_async_copy(hid.at[peer(0)[1]], xs.at[0], own_sem)
        own.start()
        greet()
        for slot in range(1, PIECES):
            send(slot).start()
        own.wait()
        keep(0).start()

    for c in range(PIECES // 2):
        @pl.when(t == c * n_tiles)
        def _(c=c):
            for slot in (2 * c, 2 * c + 1):
                if slot:
                    send(slot).wait_recv()
                    keep(slot).start()

    dim, _, hb, hd = w_ref.shape
    acc = None
    for k in range(0, dim, kp):
        turned = jnp.swapaxes(w_ref[k:k + kp, 0], 0, 1)
        cols = jnp.concatenate([turned[h] for h in range(hb)], axis=1)
        x = xs[pl.ds(2 * chunk, 2), :, k:k + kp]
        d = jnp.dot(x.reshape(-1, kp), cols, preferred_element_type=F32)
        acc = d if acc is None else acc + d
    o_ref[...] = acc.astype(BF)

    @pl.when(t == pl.num_programs(0) - 1)
    def _():
        for slot in range(PIECES):
            if slot:
                send(slot).wait_send()
            keep(slot).wait()


def gather_qkv(hidden, w, hb=8):
    pieces, tok, dim = hidden.shape
    _, kinds, heads, head_dim = w.shape
    per, width, tn = heads // hb, kinds * heads * head_dim, hb * head_dim
    n_tiles = kinds * per
    return pl.pallas_call(
        functools.partial(qkv_kernel, n_tiles=n_tiles, kp=256), name="gather_qkv", grid=(pieces // 2 * n_tiles,),
        in_specs=[ANY, pl.BlockSpec((dim, 1, hb, head_dim), lambda t: (0, t % n_tiles // per, t % per, 0))],
        out_specs=[pl.BlockSpec((2 * tok, tn), lambda t: (t // n_tiles, t % n_tiles)), ANY],
        out_shape=[jax.ShapeDtypeStruct((pieces * tok, width), BF), jax.ShapeDtypeStruct(hidden.shape, BF)],
        scratch_shapes=[pltpu.VMEM(hidden.shape, BF), pltpu.SemaphoreType.DMA, pltpu.SemaphoreType.DMA((pieces - 1,)),
                        pltpu.SemaphoreType.DMA((pieces - 1,)), pltpu.SemaphoreType.DMA((pieces,))],
        compiler_params=params(collective_id=0, has_side_effects=True))(hidden, w)


def attn_kernel(q_ref, k_ref, v_ref, qn_ref, kn_ref, o_ref, ve_ref, sc_ref, *, bq, hd, dim):
    tok = q_ref.shape[0]
    n = tok // bq
    coef = dim ** -0.5 * math.log2(math.e)

    def dot_nt(a, b):
        return lax.dot_general(a, b, (((1,), (1,)), ((), ())), preferred_element_type=F32)

    @pl.when(pl.program_id(0) == 0)
    def _():
        ve_ref[:, dim:] = jnp.zeros((tok, dim), BF)
        sc_ref[...] = dot_nt(q_ref[:bq, :dim], k_ref[:, :dim])

    def scores(g):
        h, i = divmod(g, n)
        if h < hd:
            return dot_nt(q_ref[i * bq:(i + 1) * bq, h * dim:(h + 1) * dim], k_ref[:, h * dim:(h + 1) * dim])
        return dot_nt(qn_ref[...], kn_ref[...])

    s = sc_ref[...]
    for g in range(n * hd):
        h, i = divmod(g, n)
        if i == 0:
            ve_ref[:, :dim] = v_ref[:, h * dim:(h + 1) * dim]
        ahead = scores(g + 1)
        m = jnp.max(s, axis=-1, keepdims=True)
        p = jnp.exp2((s - m) * coef)
        total = jnp.sum(p, axis=-1, keepdims=True)
        o = jnp.dot(p.astype(BF), ve_ref[...], preferred_element_type=F32)
        o_ref[i * bq:(i + 1) * bq, h * dim:(h + 1) * dim] = (o[:, :dim] * (1.0 / total)).astype(BF)
        s = ahead
    sc_ref[...] = s


def attention(qkv, heads, dim, bq=256, hd=2):
    tok = qkv.shape[0]
    steps = heads // hd
    cols = lambda j: pl.BlockSpec((tok, hd * dim), lambda t: (0, j * steps + t))
    ahead = lambda t: jnp.minimum((t + 1) * hd, heads - 1)
    return pl.pallas_call(
        functools.partial(attn_kernel, bq=bq, hd=hd, dim=dim), name="attention", grid=(steps,),
        in_specs=[cols(0), cols(1), cols(2), pl.BlockSpec((bq, dim), lambda t: (0, ahead(t))),
                  pl.BlockSpec((tok, dim), lambda t: (0, heads + ahead(t)))],
        out_specs=pl.BlockSpec((tok, hd * dim), lambda t: (0, t)),
        out_shape=jax.ShapeDtypeStruct((tok, heads * dim), BF),
        scratch_shapes=[pltpu.VMEM((tok, 2 * dim), BF), pltpu.VMEM((bq, tok), F32)],
        compiler_params=params())(*[qkv] * 5)


TANH_LIN = math.sqrt(2 / math.pi)
TANH_CUB = TANH_LIN * 0.044715


def gelu(z):
    half = 0.5 * z
    return half + half * jnp.tanh(z * (TANH_LIN + TANH_CUB * (z * z)))


def up_kernel(r_hbm, g_ref, w_ref, b_ref, o_ref, xn, rbuf, z0, z1, sem, *, tm, tn, sub, kp, ep):
    t = pl.program_id(0)
    tok, dim = xn.shape
    nm, last = tok // tm, pl.num_programs(0) - 1
    rc = rbuf.shape[1]

    @pl.when(t == 0)
    def _():
        fetch = lambda i: pltpu.make_async_copy(r_hbm.at[pl.ds(i * rc, rc)], rbuf.at[i % 2], sem.at[i % 2])
        fetch(0).start()
        gain = g_ref[...].astype(F32)
        for i in range(tok // rc):
            if i + 1 < tok // rc:
                fetch(i + 1).start()
            fetch(i).wait()

            def rows(u, _, i=i):
                at = pl.multiple_of(u * 32, 32)
                x = rbuf[i % 2, pl.ds(at, 32), :].astype(F32)
                inv = lax.rsqrt(jnp.mean(x * x, axis=-1, keepdims=True) + NORM_EPS)
                xn[pl.ds(pl.multiple_of(i * rc + at, 32), 32), :] = (x * inv * gain).astype(BF)
                return 0

            lax.fori_loop(0, rc // 32, rows, 0)

    col = jnp.maximum((t - 1) // nm, 0) * tn
    bias = lambda: b_ref[:, pl.ds(pl.multiple_of(col, tn), tn)].astype(F32)

    def tile(z_now, z_prev):
        base = pl.multiple_of(lax.rem(t, nm) * tm, tm)
        b = bias()
        parts = [(e, c) for e in range(0, tm, ep) for c in range(0, tn, sub)]
        share = len(parts) / (tm // sub * (tn // sub) * (dim // kp))
        done = step = 0
        for c in range(0, tn, sub):
            for r in range(0, tm, sub):
                acc = None
                for k in range(0, dim, kp):
                    d = jnp.dot(xn[pl.ds(base + r, sub), k:k + kp], w_ref[k:k + kp, c:c + sub], preferred_element_type=F32)
                    acc = d if acc is None else acc + d
                    step += 1
                    while done < step * share - 1e-9:
                        e, ec = parts[done]
                        done += 1
                        o_ref[e:e + ep, ec:ec + sub] = gelu(z_prev[e:e + ep, ec:ec + sub] + b[:, ec:ec + sub]).astype(BF)
                z_now[r:r + sub, c:c + sub] = acc

    for par, (za, zb) in enumerate(((z0, z1), (z1, z0))):
        @pl.when((t < last) & (lax.rem(t, 2) == par))
        def _(za=za, zb=zb):
            tile(za, zb)

    @pl.when(t == last)
    def _():
        o_ref[...] = gelu(z1[...] + bias()).astype(BF)


def norm_up(resid, gain, w, b, tm=1024, tn=1024):
    tok, dim = resid.shape
    nm = tok // tm
    tiles = nm * (w.shape[1] // tn)
    prev = lambda t: jnp.maximum(t - 1, 0)
    return pl.pallas_call(
        functools.partial(up_kernel, tm=tm, tn=tn, sub=512, kp=256, ep=32), name="norm_up", grid=(tiles + 1,),
        in_specs=[ANY, pl.BlockSpec((1, dim), lambda t: (0, 0)),
                  pl.BlockSpec((dim, tn), lambda t: (0, jnp.minimum(t, tiles - 1) // nm)),
                  pl.BlockSpec((1, w.shape[1]), lambda t: (0, 0))],
        out_specs=pl.BlockSpec((tm, tn), lambda t: (prev(t) % nm, prev(t) // nm)),
        out_shape=jax.ShapeDtypeStruct((tok, w.shape[1]), BF),
        scratch_shapes=[pltpu.VMEM((tok, dim), BF), pltpu.VMEM((2, 256, dim), BF), pltpu.VMEM((tm, tn), F32),
                        pltpu.VMEM((tm, tn), F32), pltpu.SemaphoreType.DMA((2,))],
        compiler_params=params())(resid, gain, w, b)


SLOTS = 4


def down_kernel(a_ref, w_ref, r_ref, b_ref, out, acc, obuf, own_sem, send_sem, recv_sem, *, tn, nk, nn):
    t = pl.program_id(0)
    half = PIECES // 2
    tiles = 2 * nn
    q, k = t // nk, lax.rem(t, nk)
    tok = out.shape[1]

    def moves(tile):
        far = tile < nn
        slots = range(half, PIECES) if far else range(half)
        cols = pl.ds((tile % nn) * tn, tn)
        my_row = peer(0)[1]
        for p, slot in enumerate(slots):
            src = obuf.at[tile % SLOTS, pl.ds(p * tok, tok)]
            if slot == 0:
                yield pltpu.make_async_copy(src, out.at[my_row, :, cols], own_sem.at[tile % nn]), None
            else:
                yield None, pltpu.make_async_remote_copy(
                    src_ref=src, dst_ref=out.at[my_row, :, cols], send_sem=send_sem.at[tile, p],
                    recv_sem=recv_sem.at[tile % nn, slot - 1], device_id=peer(ORDER[slot])[0],
                    device_id_type=pl.DeviceIdType.MESH)

    @pl.when(t == 0)
    def _():
        greet()

    for tile in range(tiles):
        @pl.when(t == (tile + 1) * nk)
        def _(tile=tile):
            for local, remote in moves(tile):
                (local or remote).start()

        if tile + SLOTS < tiles:
            @pl.when(t == (tile + SLOTS) * nk + nk - 1)
            def _(tile=tile):
                for local, remote in moves(tile):
                    if remote:
                        remote.wait_send()
                    else:
                        local.wait()

    @pl.when(q < tiles)
    def _():
        @pl.when(k == 0)
        def _():
            acc[...] = jnp.dot(a_ref[...], w_ref[...], preferred_element_type=F32)

        @pl.when((k > 0) & (k < nk - 1))
        def _():
            acc[...] += jnp.dot(a_ref[...], w_ref[...], preferred_element_type=F32)

        @pl.when(k == nk - 1)
        def _():
            d = jnp.dot(a_ref[...], w_ref[...], preferred_element_type=F32)
            y = r_ref[...].astype(F32) + ((acc[...] + d) + b_ref[...].astype(F32))
            obuf[lax.rem(q, SLOTS)] = y.astype(BF)

    @pl.when(q == tiles)
    def _():
        for tile in range(tiles):
            for local, remote in moves(tile):
                if tile + SLOTS >= tiles:
                    if remote:
                        remote.wait_send()
                    else:
                        local.wait()
                if remote:
                    remote.wait_recv()


def down_scatter(act, w, resid, b, tok, tn=1024, tk=4096):
    rows, kdim = act.shape
    tm, dim = rows // 2, w.shape[1]
    nn, nk = dim // tn, kdim // tk
    tiles = 2 * nn
    cur = lambda t: jnp.minimum(t, tiles * nk - 1)
    m_of = lambda t: 1 - cur(t) // (nk * nn)
    n_of = lambda t: (cur(t) // nk) % nn
    return pl.pallas_call(
        functools.partial(down_kernel, tn=tn, nk=nk, nn=nn), name="down_scatter", grid=(tiles * nk + 1,),
        in_specs=[pl.BlockSpec((tm, tk), lambda t: (m_of(t), cur(t) % nk)),
                  pl.BlockSpec((tk, tn), lambda t: (cur(t) % nk, n_of(t))),
                  pl.BlockSpec((tm, tn), lambda t: (m_of(t), n_of(t))), pl.BlockSpec((1, tn), lambda t: (0, n_of(t)))],
        out_specs=ANY, out_shape=jax.ShapeDtypeStruct((PIECES, tok, dim), BF),
        scratch_shapes=[pltpu.VMEM((tm, tn), F32), pltpu.VMEM((SLOTS, tm, tn), BF), pltpu.SemaphoreType.DMA((nn,)),
                        pltpu.SemaphoreType.DMA((tiles, PIECES // 2)), pltpu.SemaphoreType.DMA((nn, PIECES - 1))],
        compiler_params=params(collective_id=1, has_side_effects=True))(act, w, resid, b)


def solution(mesh):
    tok_spec = P("dp", ("cp", "sp"), None)

    def local_block(hidden, w_qkv, w_out, norm_gain, w_up, b_up, w_down, b_down):
        pieces, tok, dim = hidden.shape
        _, _, heads, head_dim = w_qkv.shape
        qkv, row = gather_qkv(hidden, w_qkv)
        attn = attention(qkv, heads, head_dim)
        attn_out = jnp.dot(attn, w_out.reshape(heads * head_dim, dim), preferred_element_type=F32).astype(BF)
        resid = (row.reshape(pieces * tok, dim).astype(F32) + attn_out.astype(F32)).astype(BF)
        act = norm_up(resid, norm_gain.reshape(1, dim), w_up, b_up.reshape(1, -1))
        return down_scatter(act, w_down, resid, b_down.reshape(1, dim), tok)

    return jax.shard_map(local_block, mesh=mesh, in_specs=(tok_spec, P(), P(), P(), P(), P(), P(), P()), out_specs=tok_spec, check_vma=False)
```

```python
import functools
import math

import jax
import jax.numpy as jnp
from jax import lax
from jax.experimental import pallas as pl
from jax.experimental.pallas import tpu as pltpu
from jax.sharding import PartitionSpec as P

NORM_EPS = 1e-6
VMEM_BYTES = 63 * 2**20
BF = jnp.bfloat16
F32 = jnp.float32
ANY = pl.BlockSpec(memory_space=pl.ANY)

ORDER = (0, 2, 4, 1, 6, 3, 5, 7)
PIECES = 8


def peer(rel):
    i, j = lax.axis_index("cp"), lax.axis_index("sp")
    kx, kc, ky = rel // 4, (rel // 2) % 2, rel % 2
    x = lax.rem(i // 2 + kx, 2)
    core = lax.rem(lax.rem(i, 2) + kc, 2)
    cp, sp = x * 2 + core, lax.rem(j + ky, 2)
    return {"cp": cp, "sp": sp}, cp * 2 + sp


def arrive():
    bar = pltpu.get_barrier_semaphore()
    for rel in range(1, PIECES):
        pl.semaphore_signal(bar, inc=1, device_id=peer(rel)[0], device_id_type=pl.DeviceIdType.MESH)


def await_all():
    pl.semaphore_wait(pltpu.get_barrier_semaphore(), PIECES - 1)


def params(**kw):
    return pltpu.CompilerParams(vmem_limit_bytes=VMEM_BYTES, **kw)


def qkv_kernel(hid, w_hbm, o_ref, row_out, xs, wbuf, w_sem, own_sem, send_sem, recv_sem, out_sem, *, n_tiles, kp, group):
    t = pl.program_id(0)
    last = pl.num_programs(0) - 1
    chunk = t // n_tiles
    dim, hb, hd = wbuf.shape[1:]
    per = n_tiles // w_hbm.shape[1]

    def weights(step):
        tile = lax.rem(step, n_tiles)
        heads = pl.ds(pl.multiple_of(lax.rem(tile, per) * hb, hb), hb)
        return pltpu.make_async_copy(w_hbm.at[:, tile // per, heads], wbuf.at[lax.rem(step, 2)], w_sem.at[lax.rem(step, 2)])

    def send(slot):
        dev, row = peer(ORDER[slot])
        return pltpu.make_async_remote_copy(
            src_ref=hid.at[row], dst_ref=xs.at[slot], send_sem=send_sem.at[slot - 1], recv_sem=recv_sem.at[slot - 1],
            device_id=dev, device_id_type=pl.DeviceIdType.MESH)

    def keep(slot):
        return pltpu.make_async_copy(xs.at[slot], row_out.at[slot], out_sem.at[slot])

    @pl.when(t == 0)
    def _():
        own = pltpu.make_async_copy(hid.at[peer(0)[1]], xs.at[0], own_sem)
        own.start()
        weights(t).start()
        arrive()
        await_all()
        for slot in range(1, PIECES):
            send(slot).start()
        own.wait()
        keep(0).start()

    for c in range(PIECES // 2):
        @pl.when(t == c * n_tiles)
        def _(c=c):
            for slot in (2 * c, 2 * c + 1):
                if slot:
                    send(slot).wait_recv()
                    keep(slot).start()

    @pl.when(t < last)
    def _():
        weights(t + 1).start()

    weights(t).wait()

    w_ref = wbuf.at[lax.rem(t, 2)]
    for h in range(0, hb, group):
        acc = None
        for k in range(0, dim, kp):
            turned = jnp.swapaxes(w_ref[k:k + kp, h:h + group], 0, 1)
            cols = jnp.concatenate([turned[g] for g in range(group)], axis=1)
            x = xs[pl.ds(2 * chunk, 2), :, k:k + kp]
            d = jnp.dot(x.reshape(-1, kp), cols, preferred_element_type=F32)
            acc = d if acc is None else acc + d
        o_ref[:, h * hd:(h + group) * hd] = acc.astype(BF)

    @pl.when(t == last)
    def _():
        for slot in range(PIECES):
            if slot:
                send(slot).wait_send()
            keep(slot).wait()


def gather_qkv(hidden, w, hb=16):
    pieces, tok, dim = hidden.shape
    _, kinds, heads, head_dim = w.shape
    per, width, tn = heads // hb, kinds * heads * head_dim, hb * head_dim
    n_tiles = kinds * per
    return pl.pallas_call(
        functools.partial(qkv_kernel, n_tiles=n_tiles, kp=256, group=8), name="gather_qkv", grid=(pieces // 2 * n_tiles,),
        in_specs=[ANY, ANY],
        out_specs=[pl.BlockSpec((2 * tok, tn), lambda t: (t // n_tiles, t % n_tiles)), ANY],
        out_shape=[jax.ShapeDtypeStruct((pieces * tok, width), BF), jax.ShapeDtypeStruct(hidden.shape, BF)],
        scratch_shapes=[pltpu.VMEM(hidden.shape, BF), pltpu.VMEM((2, dim, hb, head_dim), BF), pltpu.SemaphoreType.DMA((2,)),
                        pltpu.SemaphoreType.DMA, pltpu.SemaphoreType.DMA((pieces - 1,)),
                        pltpu.SemaphoreType.DMA((pieces - 1,)), pltpu.SemaphoreType.DMA((pieces,))],
        compiler_params=params(collective_id=0, has_side_effects=True))(hidden, w)


def attn_kernel(q_ref, k_ref, v_ref, qn_ref, kn_ref, o_ref, ve_ref, sc_ref, *, bq, hd, dim):
    tok = q_ref.shape[0]
    n = tok // bq
    coef = dim ** -0.5 * math.log2(math.e)

    def dot_nt(a, b):
        return lax.dot_general(a, b, (((1,), (1,)), ((), ())), preferred_element_type=F32)

    @pl.when(pl.program_id(0) == 0)
    def _():
        ve_ref[:, dim:] = jnp.zeros((tok, dim), BF)
        sc_ref[...] = dot_nt(q_ref[:bq, :dim], k_ref[:, :dim])

    def scores(g):
        h, i = divmod(g, n)
        if h < hd:
            return dot_nt(q_ref[i * bq:(i + 1) * bq, h * dim:(h + 1) * dim], k_ref[:, h * dim:(h + 1) * dim])
        return dot_nt(qn_ref[...], kn_ref[...])

    s = sc_ref[...]
    for g in range(n * hd):
        h, i = divmod(g, n)
        if i == 0:
            ve_ref[:, :dim] = v_ref[:, h * dim:(h + 1) * dim]
        ahead = scores(g + 1)
        m = jnp.max(s, axis=-1, keepdims=True)
        p = jnp.exp2((s - m) * coef)
        total = jnp.sum(p, axis=-1, keepdims=True)
        o = jnp.dot(p.astype(BF), ve_ref[...], preferred_element_type=F32)
        o_ref[i * bq:(i + 1) * bq, h * dim:(h + 1) * dim] = (o[:, :dim] * (1.0 / total)).astype(BF)
        s = ahead
    sc_ref[...] = s


def attention(qkv, heads, dim, bq=256, hd=2):
    tok = qkv.shape[0]
    steps = heads // hd
    cols = lambda j: pl.BlockSpec((tok, hd * dim), lambda t: (0, j * steps + t))
    ahead = lambda t: jnp.minimum((t + 1) * hd, heads - 1)
    return pl.pallas_call(
        functools.partial(attn_kernel, bq=bq, hd=hd, dim=dim), name="attention", grid=(steps,),
        in_specs=[cols(0), cols(1), cols(2), pl.BlockSpec((bq, dim), lambda t: (0, ahead(t))),
                  pl.BlockSpec((tok, dim), lambda t: (0, heads + ahead(t)))],
        out_specs=pl.BlockSpec((tok, hd * dim), lambda t: (0, t)),
        out_shape=jax.ShapeDtypeStruct((tok, heads * dim), BF),
        scratch_shapes=[pltpu.VMEM((tok, 2 * dim), BF), pltpu.VMEM((bq, tok), F32)],
        compiler_params=params())(*[qkv] * 5)


TANH_LIN = math.sqrt(2 / math.pi)
TANH_CUB = TANH_LIN * 0.044715


def gelu(z):
    half = 0.5 * z
    return half + half * jnp.tanh(z * (TANH_LIN + TANH_CUB * (z * z)))


def up_kernel(r_hbm, v_ref, w_ref, o_ref, xn, rbuf, z0, z1, sem, *, tm, tn, sub, kp, ep, rn):
    t = pl.program_id(0)
    tok, dim = xn.shape
    nm, last = tok // tm, pl.num_programs(0) - 1
    rc = rbuf.shape[1]

    @pl.when(t == 0)
    def _():
        fetch = lambda i: pltpu.make_async_copy(r_hbm.at[pl.ds(i * rc, rc)], rbuf.at[i % 2], sem.at[i % 2])
        fetch(0).start()
        gain = v_ref[:, :dim].astype(F32)
        for i in range(tok // rc):
            if i + 1 < tok // rc:
                fetch(i + 1).start()
            fetch(i).wait()

            def rows(u, _, i=i):
                at = pl.multiple_of(u * rn, rn)
                x = rbuf[i % 2, pl.ds(at, rn), :].astype(F32)
                inv = lax.rsqrt(jnp.mean(x * x, axis=-1, keepdims=True) + NORM_EPS)
                xn[pl.ds(pl.multiple_of(i * rc + at, rn), rn), :] = (x * inv * gain).astype(BF)
                return 0

            lax.fori_loop(0, rc // rn, rows, 0)

    col = jnp.maximum((t - 1) // nm, 0) * tn
    bias = lambda: v_ref[:, pl.ds(pl.multiple_of(dim + col, tn), tn)].astype(F32)

    def tile(z_now, z_prev):
        base = pl.multiple_of(lax.rem(t, nm) * tm, tm)
        b = bias()
        parts = [(e, c) for e in range(0, tm, ep) for c in range(0, tn, sub)]
        share = len(parts) / (tm // sub * (tn // sub) * (dim // kp))
        done = step = 0
        for c in range(0, tn, sub):
            for r in range(0, tm, sub):
                acc = None
                for k in range(0, dim, kp):
                    d = jnp.dot(xn[pl.ds(base + r, sub), k:k + kp], w_ref[k:k + kp, c:c + sub], preferred_element_type=F32)
                    acc = d if acc is None else acc + d
                    step += 1
                    while done < step * share - 1e-9:
                        e, ec = parts[done]
                        done += 1
                        o_ref[e:e + ep, ec:ec + sub] = gelu(z_prev[e:e + ep, ec:ec + sub] + b[:, ec:ec + sub]).astype(BF)
                z_now[r:r + sub, c:c + sub] = acc

    for par, (za, zb) in enumerate(((z0, z1), (z1, z0))):
        @pl.when((t < last) & (lax.rem(t, 2) == par))
        def _(za=za, zb=zb):
            tile(za, zb)

    @pl.when(t == last)
    def _():
        o_ref[...] = gelu(z1[...] + bias()).astype(BF)


def norm_up(resid, vec, w, tm=1024, tn=1024):
    tok, dim = resid.shape
    nm = tok // tm
    tiles = nm * (w.shape[1] // tn)
    prev = lambda t: jnp.maximum(t - 1, 0)
    return pl.pallas_call(
        functools.partial(up_kernel, tm=tm, tn=tn, sub=512, kp=256, ep=32, rn=128), name="norm_up", grid=(tiles + 1,),
        in_specs=[ANY, pl.BlockSpec(vec.shape, lambda t: (0, 0)),
                  pl.BlockSpec((dim, tn), lambda t: (0, jnp.minimum(t, tiles - 1) // nm))],
        out_specs=pl.BlockSpec((tm, tn), lambda t: (prev(t) % nm, prev(t) // nm)),
        out_shape=jax.ShapeDtypeStruct((tok, w.shape[1]), BF),
        scratch_shapes=[pltpu.VMEM((tok, dim), BF), pltpu.VMEM((2, 256, dim), BF), pltpu.VMEM((tm, tn), F32),
                        pltpu.VMEM((tm, tn), F32), pltpu.SemaphoreType.DMA((2,))],
        compiler_params=params())(resid, vec, w)


SLOTS = 3


def down_kernel(a_ref, w_ref, r_ref, b_ref, out, acc, obuf, own_sem, send_sem, recv_sem, *, tn, nk, nn):
    t = pl.program_id(0)
    tiles = PIECES // 2 * nn
    q, k = t // nk, lax.rem(t, nk)
    tok = out.shape[1]

    def moves(tile):
        chunk = PIECES // 2 - 1 - tile // nn
        cols = pl.ds(tile % nn * tn, tn)
        my_row = peer(0)[1]
        for p in range(2):
            slot = 2 * chunk + p
            src = obuf.at[tile % SLOTS, pl.ds(p * tok, tok)]
            dst = out.at[my_row, :, cols]
            if slot == 0:
                yield pltpu.make_async_copy(src, dst, own_sem.at[tile % nn]), None
            else:
                yield None, pltpu.make_async_remote_copy(
                    src_ref=src, dst_ref=dst, send_sem=send_sem.at[tile, p], recv_sem=recv_sem.at[tile % nn, slot - 1],
                    device_id=peer(ORDER[slot])[0], device_id_type=pl.DeviceIdType.MESH)

    def sent(tile):
        for local, remote in moves(tile):
            if remote:
                remote.wait_send()
            else:
                local.wait()

    @pl.when(t == 0)
    def _():
        arrive()

    @pl.when(t == nk)
    def _():
        await_all()

    for tile in range(tiles):
        @pl.when(t == (tile + 1) * nk)
        def _(tile=tile):
            for local, remote in moves(tile):
                (local or remote).start()

        if tile + SLOTS < tiles:
            @pl.when(t == (tile + SLOTS) * nk + nk - 1)
            def _(tile=tile):
                sent(tile)

    @pl.when(q < tiles)
    def _():
        @pl.when(k == 0)
        def _():
            acc[...] = jnp.dot(a_ref[...], w_ref[...], preferred_element_type=F32)

        @pl.when((k > 0) & (k < nk - 1))
        def _():
            acc[...] += jnp.dot(a_ref[...], w_ref[...], preferred_element_type=F32)

        @pl.when(k == nk - 1)
        def _():
            d = jnp.dot(a_ref[...], w_ref[...], preferred_element_type=F32)
            y = r_ref[...].astype(F32) + ((acc[...] + d) + b_ref[...].astype(F32))
            obuf[lax.rem(q, SLOTS)] = y.astype(BF)

    @pl.when(q == tiles)
    def _():
        for tile in range(tiles - SLOTS, tiles):
            sent(tile)
        for tile in range(tiles):
            for _, remote in moves(tile):
                if remote:
                    remote.wait_recv()


def down_scatter(act, w, resid, b, tok, tn=2048, tk=4096):
    rows, kdim = act.shape
    dim = w.shape[1]
    tm, nn, nk = 2 * tok, dim // tn, kdim // tk
    tiles = PIECES // 2 * nn
    cur = lambda t: jnp.minimum(t, tiles * nk - 1)
    m_of = lambda t: PIECES // 2 - 1 - cur(t) // (nk * nn)
    n_of = lambda t: (cur(t) // nk) % nn
    return pl.pallas_call(
        functools.partial(down_kernel, tn=tn, nk=nk, nn=nn), name="down_scatter", grid=(tiles * nk + 1,),
        in_specs=[pl.BlockSpec((tm, tk), lambda t: (m_of(t), cur(t) % nk)),
                  pl.BlockSpec((tk, tn), lambda t: (cur(t) % nk, n_of(t))),
                  pl.BlockSpec((tm, tn), lambda t: (m_of(t), n_of(t))),
                  pl.BlockSpec((1, tn), lambda t: (0, b.shape[1] // tn - nn + n_of(t)))],
        out_specs=ANY, out_shape=jax.ShapeDtypeStruct((PIECES, tok, dim), BF),
        scratch_shapes=[pltpu.VMEM((tm, tn), F32), pltpu.VMEM((SLOTS, tm, tn), BF), pltpu.SemaphoreType.DMA((nn,)),
                        pltpu.SemaphoreType.DMA((tiles, 2)), pltpu.SemaphoreType.DMA((nn, PIECES - 1))],
        compiler_params=params(collective_id=1, has_side_effects=True))(act, w, resid, b)


def settle_kernel(x, out, buf, in_sem, out_sem):
    load = [pltpu.make_async_copy(x.at[i], buf.at[i], in_sem.at[i]) for i in range(PIECES)]
    save = [pltpu.make_async_copy(buf.at[i], out.at[i], out_sem.at[i]) for i in range(PIECES)]
    for c in load:
        c.start()
    for a, b in zip(load, save):
        a.wait()
        b.start()
    for c in save:
        c.wait()


def settle(x):
    return pl.pallas_call(
        settle_kernel, name="settle", in_specs=[ANY], out_specs=ANY, out_shape=jax.ShapeDtypeStruct(x.shape, x.dtype),
        scratch_shapes=[pltpu.VMEM(x.shape, x.dtype), pltpu.SemaphoreType.DMA((PIECES,)), pltpu.SemaphoreType.DMA((PIECES,))],
        compiler_params=params())(x)


def solution(mesh):
    tok_spec = P("dp", ("cp", "sp"), None)

    def local_block(hidden, w_qkv, w_out, norm_gain, w_up, b_up, w_down, b_down):
        pieces, tok, dim = hidden.shape
        _, _, heads, head_dim = w_qkv.shape
        qkv, row = gather_qkv(hidden, w_qkv)
        attn = attention(qkv, heads, head_dim)
        attn_out = jnp.dot(attn, w_out.reshape(heads * head_dim, dim), preferred_element_type=F32).astype(BF)
        resid = (row.reshape(pieces * tok, dim).astype(F32) + attn_out.astype(F32)).astype(BF)
        vec = jnp.concatenate([norm_gain, b_up, b_down]).reshape(1, -1)
        act = norm_up(resid, vec, w_up)
        return settle(down_scatter(act, w_down, resid, vec, tok))

    return jax.shard_map(local_block, mesh=mesh, in_specs=(tok_spec, P(), P(), P(), P(), P(), P(), P()), out_specs=tok_spec, check_vma=False)
```

```python
import functools
import math

import jax
import jax.numpy as jnp
from jax import lax
from jax.experimental import pallas as pl
from jax.experimental.pallas import tpu as pltpu
from jax.sharding import PartitionSpec as P

NORM_EPS = 1e-6
VMEM_BYTES = 63 * 2**20
BF = jnp.bfloat16
F32 = jnp.float32
ANY = pl.BlockSpec(memory_space=pl.ANY)

ORDER = (0, 2, 4, 1, 6, 3, 5, 7)
PIECES = 8


def peer(rel):
    i, j = lax.axis_index("cp"), lax.axis_index("sp")
    kx, kc, ky = rel // 4, (rel // 2) % 2, rel % 2
    x = lax.rem(i // 2 + kx, 2)
    core = lax.rem(lax.rem(i, 2) + kc, 2)
    cp, sp = x * 2 + core, lax.rem(j + ky, 2)
    return {"cp": cp, "sp": sp}, cp * 2 + sp


def arrive():
    bar = pltpu.get_barrier_semaphore()
    for rel in range(1, PIECES):
        pl.semaphore_signal(bar, inc=1, device_id=peer(rel)[0], device_id_type=pl.DeviceIdType.MESH)


def await_all():
    pl.semaphore_wait(pltpu.get_barrier_semaphore(), PIECES - 1)


def params(**kw):
    return pltpu.CompilerParams(vmem_limit_bytes=VMEM_BYTES, **kw)


def qkv_kernel(hid, w_hbm, o_ref, row_out, xs, wbuf, w_sem, own_sem, send_sem, recv_sem, out_sem, *, n_tiles, kp, group):
    t = pl.program_id(0)
    last = pl.num_programs(0) - 1
    chunk = t // n_tiles
    dim, hb, hd = wbuf.shape[1:]
    per = n_tiles // w_hbm.shape[1]

    def weights(step):
        tile = lax.rem(step, n_tiles)
        heads = pl.ds(pl.multiple_of(lax.rem(tile, per) * hb, hb), hb)
        return pltpu.make_async_copy(w_hbm.at[:, tile // per, heads], wbuf.at[lax.rem(step, 2)], w_sem.at[lax.rem(step, 2)])

    def send(slot):
        dev, row = peer(ORDER[slot])
        return pltpu.make_async_remote_copy(
            src_ref=hid.at[row], dst_ref=xs.at[slot], send_sem=send_sem.at[slot - 1], recv_sem=recv_sem.at[slot - 1],
            device_id=dev, device_id_type=pl.DeviceIdType.MESH)

    def keep(slot):
        return pltpu.make_async_copy(xs.at[slot], row_out.at[slot], out_sem.at[slot])

    @pl.when(t == 0)
    def _():
        own = pltpu.make_async_copy(hid.at[peer(0)[1]], xs.at[0], own_sem)
        own.start()
        weights(t).start()
        arrive()
        await_all()
        for slot in range(1, PIECES):
            send(slot).start()
        own.wait()
        keep(0).start()

    for c in range(PIECES // 2):
        @pl.when(t == c * n_tiles)
        def _(c=c):
            for slot in (2 * c, 2 * c + 1):
                if slot:
                    send(slot).wait_recv()
                    keep(slot).start()

    @pl.when(t < last)
    def _():
        weights(t + 1).start()

    weights(t).wait()

    w_ref = wbuf.at[lax.rem(t, 2)]
    for h in range(0, hb, group):
        acc = None
        for k in range(0, dim, kp):
            turned = jnp.swapaxes(w_ref[k:k + kp, h:h + group], 0, 1)
            cols = jnp.concatenate([turned[g] for g in range(group)], axis=1)
            x = xs[pl.ds(2 * chunk, 2), :, k:k + kp]
            d = jnp.dot(x.reshape(-1, kp), cols, preferred_element_type=F32)
            acc = d if acc is None else acc + d
        o_ref[:, h * hd:(h + group) * hd] = acc.astype(BF)

    @pl.when(t == last)
    def _():
        for slot in range(PIECES):
            if slot:
                send(slot).wait_send()
            keep(slot).wait()


def gather_qkv(hidden, w, hb=16):
    pieces, tok, dim = hidden.shape
    _, kinds, heads, head_dim = w.shape
    per, width, tn = heads // hb, kinds * heads * head_dim, hb * head_dim
    n_tiles = kinds * per
    return pl.pallas_call(
        functools.partial(qkv_kernel, n_tiles=n_tiles, kp=256, group=8), name="gather_qkv", grid=(pieces // 2 * n_tiles,),
        in_specs=[ANY, ANY],
        out_specs=[pl.BlockSpec((2 * tok, tn), lambda t: (t // n_tiles, t % n_tiles)), ANY],
        out_shape=[jax.ShapeDtypeStruct((pieces * tok, width), BF), jax.ShapeDtypeStruct(hidden.shape, BF)],
        scratch_shapes=[pltpu.VMEM(hidden.shape, BF), pltpu.VMEM((2, dim, hb, head_dim), BF), pltpu.SemaphoreType.DMA((2,)),
                        pltpu.SemaphoreType.DMA, pltpu.SemaphoreType.DMA((pieces - 1,)),
                        pltpu.SemaphoreType.DMA((pieces - 1,)), pltpu.SemaphoreType.DMA((pieces,))],
        compiler_params=params(collective_id=0, has_side_effects=True))(hidden, w)


def attn_kernel(q_ref, k_ref, v_ref, qn_ref, kn_ref, o_ref, ve_ref, sc_ref, *, bq, hd, dim):
    tok = q_ref.shape[0]
    n = tok // bq
    coef = dim ** -0.5 * math.log2(math.e)

    def dot_nt(a, b):
        return lax.dot_general(a, b, (((1,), (1,)), ((), ())), preferred_element_type=F32)

    @pl.when(pl.program_id(0) == 0)
    def _():
        ve_ref[:, dim:] = jnp.zeros((tok, dim), BF)
        sc_ref[...] = dot_nt(q_ref[:bq, :dim], k_ref[:, :dim])

    def scores(g):
        h, i = divmod(g, n)
        if h < hd:
            return dot_nt(q_ref[i * bq:(i + 1) * bq, h * dim:(h + 1) * dim], k_ref[:, h * dim:(h + 1) * dim])
        return dot_nt(qn_ref[...], kn_ref[...])

    s = sc_ref[...]
    for g in range(n * hd):
        h, i = divmod(g, n)
        if i == 0:
            ve_ref[:, :dim] = v_ref[:, h * dim:(h + 1) * dim]
        ahead = scores(g + 1)
        m = jnp.max(s, axis=-1, keepdims=True)
        p = jnp.exp2((s - m) * coef)
        total = jnp.sum(p, axis=-1, keepdims=True)
        o = jnp.dot(p.astype(BF), ve_ref[...], preferred_element_type=F32)
        o_ref[i * bq:(i + 1) * bq, h * dim:(h + 1) * dim] = (o[:, :dim] * (1.0 / total)).astype(BF)
        s = ahead
    sc_ref[...] = s


def attention(qkv, heads, dim, bq=256, hd=4):
    tok = qkv.shape[0]
    steps = heads // hd
    cols = lambda j: pl.BlockSpec((tok, hd * dim), lambda t: (0, j * steps + t))
    ahead = lambda t: jnp.minimum((t + 1) * hd, heads - 1)
    return pl.pallas_call(
        functools.partial(attn_kernel, bq=bq, hd=hd, dim=dim), name="attention", grid=(steps,),
        in_specs=[cols(0), cols(1), cols(2), pl.BlockSpec((bq, dim), lambda t: (0, ahead(t))),
                  pl.BlockSpec((tok, dim), lambda t: (0, heads + ahead(t)))],
        out_specs=pl.BlockSpec((tok, hd * dim), lambda t: (0, t)),
        out_shape=jax.ShapeDtypeStruct((tok, heads * dim), BF),
        scratch_shapes=[pltpu.VMEM((tok, 2 * dim), BF), pltpu.VMEM((bq, tok), F32)],
        compiler_params=params())(*[qkv] * 5)


TANH_LIN = math.sqrt(2 / math.pi)
TANH_CUB = TANH_LIN * 0.044715


def gelu(z):
    half = 0.5 * z
    return half + half * jnp.tanh(z * (TANH_LIN + TANH_CUB * (z * z)))


def up_kernel(r_hbm, v_ref, w_hbm, o_ref, xn, rbuf, z0, z1, wbuf, w_sem, sem, *, tm, tn, sub, kp, ep, rn):
    t = pl.program_id(0)
    tok, dim = xn.shape
    nm, last = tok // tm, pl.num_programs(0) - 1
    rc = rbuf.shape[1]

    def weights(n):
        cols = pl.ds(pl.multiple_of(n * tn, tn), tn)
        return pltpu.make_async_copy(w_hbm.at[:, cols], wbuf.at[lax.rem(n, 2)], w_sem.at[lax.rem(n, 2)])

    @pl.when(t == 0)
    def _():
        fetch = lambda i: pltpu.make_async_copy(r_hbm.at[pl.ds(i * rc, rc)], rbuf.at[lax.rem(i, 2)], sem.at[lax.rem(i, 2)])
        fetch(0).start()
        weights(0).start()
        gain = v_ref[:, :dim].astype(F32)

        def block(i, _):
            @pl.when(i + 1 < tok // rc)
            def _():
                fetch(i + 1).start()

            fetch(i).wait()

            def rows(u, _):
                at = pl.multiple_of(u * rn, rn)
                x = rbuf[lax.rem(i, 2), pl.ds(at, rn), :].astype(F32)
                inv = lax.rsqrt(jnp.mean(x * x, axis=-1, keepdims=True) + NORM_EPS)
                xn[pl.ds(pl.multiple_of(i * rc + at, rn), rn), :] = (x * inv * gain).astype(BF)
                return 0

            return lax.fori_loop(0, rc // rn, rows, 0)

        lax.fori_loop(0, tok // rc, block, 0)

    n = t // nm

    @pl.when((t < last) & (lax.rem(t, nm) == 0))
    def _():
        @pl.when(t + nm < last)
        def _():
            weights(n + 1).start()

        weights(n).wait()

    w_ref = wbuf.at[lax.rem(n, 2)]
    col = jnp.maximum((t - 1) // nm, 0) * tn
    bias = lambda: v_ref[:, pl.ds(pl.multiple_of(dim + col, tn), tn)].astype(F32)

    def tile(z_now, z_prev):
        base = pl.multiple_of(lax.rem(t, nm) * tm, tm)
        b = bias()
        parts = [(e, c) for e in range(0, tm, ep) for c in range(0, tn, sub)]
        share = len(parts) / (tm // sub * (tn // sub) * (dim // kp))
        done = step = 0
        for c in range(0, tn, sub):
            for r in range(0, tm, sub):
                acc = None
                for k in range(0, dim, kp):
                    d = jnp.dot(xn[pl.ds(base + r, sub), k:k + kp], w_ref[k:k + kp, c:c + sub], preferred_element_type=F32)
                    acc = d if acc is None else acc + d
                    step += 1
                    while done < step * share - 1e-9:
                        e, ec = parts[done]
                        done += 1
                        o_ref[e:e + ep, ec:ec + sub] = gelu(z_prev[e:e + ep, ec:ec + sub] + b[:, ec:ec + sub]).astype(BF)
                z_now[r:r + sub, c:c + sub] = acc

    for par, (za, zb) in enumerate(((z0, z1), (z1, z0))):
        @pl.when((t < last) & (lax.rem(t, 2) == par))
        def _(za=za, zb=zb):
            tile(za, zb)

    @pl.when(t == last)
    def _():
        o_ref[...] = gelu(z1[...] + bias()).astype(BF)


def norm_up(resid, vec, w, tm=1024, tn=1024):
    tok, dim = resid.shape
    nm = tok // tm
    tiles = nm * (w.shape[1] // tn)
    prev = lambda t: jnp.maximum(t - 1, 0)
    return pl.pallas_call(
        functools.partial(up_kernel, tm=tm, tn=tn, sub=512, kp=256, ep=32, rn=128), name="norm_up", grid=(tiles + 1,),
        in_specs=[ANY, pl.BlockSpec(vec.shape, lambda t: (0, 0)), ANY],
        out_specs=pl.BlockSpec((tm, tn), lambda t: (prev(t) % nm, prev(t) // nm)),
        out_shape=jax.ShapeDtypeStruct((tok, w.shape[1]), BF),
        scratch_shapes=[pltpu.VMEM((tok, dim), BF), pltpu.VMEM((2, 256, dim), BF), pltpu.VMEM((tm, tn), F32),
                        pltpu.VMEM((tm, tn), F32), pltpu.VMEM((2, dim, tn), BF), pltpu.SemaphoreType.DMA((2,)),
                        pltpu.SemaphoreType.DMA((2,))],
        compiler_params=params())(resid, vec, w)


SLOTS = 3


def down_kernel(a_ref, w_ref, r_ref, b_ref, out, acc, obuf, own_sem, send_sem, recv_sem, *, tn, nk, nn):
    t = pl.program_id(0)
    tiles = PIECES // 2 * nn
    q, k = t // nk, lax.rem(t, nk)
    tok = out.shape[1]

    def moves(tile):
        chunk = PIECES // 2 - 1 - tile // nn
        cols = pl.ds(tile % nn * tn, tn)
        my_row = peer(0)[1]
        for p in range(2):
            slot = 2 * chunk + p
            src = obuf.at[tile % SLOTS, pl.ds(p * tok, tok)]
            dst = out.at[my_row, :, cols]
            if slot == 0:
                yield pltpu.make_async_copy(src, dst, own_sem.at[tile % nn]), None
            else:
                yield None, pltpu.make_async_remote_copy(
                    src_ref=src, dst_ref=dst, send_sem=send_sem.at[tile, p], recv_sem=recv_sem.at[tile % nn, slot - 1],
                    device_id=peer(ORDER[slot])[0], device_id_type=pl.DeviceIdType.MESH)

    def sent(tile):
        for local, remote in moves(tile):
            if remote:
                remote.wait_send()
            else:
                local.wait()

    @pl.when(t == 0)
    def _():
        arrive()

    @pl.when(t == nk)
    def _():
        await_all()

    for tile in range(tiles):
        @pl.when(t == (tile + 1) * nk)
        def _(tile=tile):
            for local, remote in moves(tile):
                (local or remote).start()

        if tile + SLOTS < tiles:
            @pl.when(t == (tile + SLOTS) * nk + nk - 1)
            def _(tile=tile):
                sent(tile)

    @pl.when(q < tiles)
    def _():
        @pl.when(k < nk - 1)
        def _():
            d = jnp.dot(a_ref[...], w_ref[...], preferred_element_type=F32)
            acc[...] = jnp.where(k == 0, d, acc[...] + d)

        @pl.when(k == nk - 1)
        def _():
            d = jnp.dot(a_ref[...], w_ref[...], preferred_element_type=F32)
            y = r_ref[...].astype(F32) + ((acc[...] + d) + b_ref[...].astype(F32))
            obuf[lax.rem(q, SLOTS)] = y.astype(BF)

    @pl.when(q == tiles)
    def _():
        for tile in range(tiles - SLOTS, tiles):
            sent(tile)
        for tile in range(tiles):
            for _, remote in moves(tile):
                if remote:
                    remote.wait_recv()


def down_scatter(act, w, resid, b, tok, tn=2048, tk=4096):
    rows, kdim = act.shape
    dim = w.shape[1]
    tm, nn, nk = 2 * tok, dim // tn, kdim // tk
    tiles = PIECES // 2 * nn
    cur = lambda t: jnp.minimum(t, tiles * nk - 1)
    m_of = lambda t: PIECES // 2 - 1 - cur(t) // (nk * nn)
    n_of = lambda t: (cur(t) // nk) % nn
    return pl.pallas_call(
        functools.partial(down_kernel, tn=tn, nk=nk, nn=nn), name="down_scatter", grid=(tiles * nk + 1,),
        in_specs=[pl.BlockSpec((tm, tk), lambda t: (m_of(t), cur(t) % nk)),
                  pl.BlockSpec((tk, tn), lambda t: (cur(t) % nk, n_of(t))),
                  pl.BlockSpec((tm, tn), lambda t: (m_of(t), n_of(t))),
                  pl.BlockSpec((1, tn), lambda t: (0, b.shape[1] // tn - nn + n_of(t)))],
        out_specs=ANY, out_shape=jax.ShapeDtypeStruct((PIECES, tok, dim), BF),
        scratch_shapes=[pltpu.VMEM((tm, tn), F32), pltpu.VMEM((SLOTS, tm, tn), BF), pltpu.SemaphoreType.DMA((nn,)),
                        pltpu.SemaphoreType.DMA((tiles, 2)), pltpu.SemaphoreType.DMA((nn, PIECES - 1))],
        compiler_params=params(collective_id=1, has_side_effects=True))(act, w, resid, b)


def settle_kernel(x, out, buf, in_sem, out_sem):
    load = [pltpu.make_async_copy(x.at[i], buf.at[i], in_sem.at[i]) for i in range(PIECES)]
    save = [pltpu.make_async_copy(buf.at[i], out.at[i], out_sem.at[i]) for i in range(PIECES)]
    for c in load:
        c.start()
    for a, b in zip(load, save):
        a.wait()
        b.start()
    for c in save:
        c.wait()


def settle(x):
    return pl.pallas_call(
        settle_kernel, name="settle", in_specs=[ANY], out_specs=ANY, out_shape=jax.ShapeDtypeStruct(x.shape, x.dtype),
        scratch_shapes=[pltpu.VMEM(x.shape, x.dtype), pltpu.SemaphoreType.DMA((PIECES,)), pltpu.SemaphoreType.DMA((PIECES,))],
        compiler_params=params())(x)


def solution(mesh):
    tok_spec = P("dp", ("cp", "sp"), None)

    def local_block(hidden, w_qkv, w_out, norm_gain, w_up, b_up, w_down, b_down):
        pieces, tok, dim = hidden.shape
        _, _, heads, head_dim = w_qkv.shape
        qkv, row = gather_qkv(hidden, w_qkv)
        attn = attention(qkv, heads, head_dim)
        attn_out = jnp.dot(attn, w_out.reshape(heads * head_dim, dim), preferred_element_type=F32).astype(BF)
        resid = (row.reshape(pieces * tok, dim).astype(F32) + attn_out.astype(F32)).astype(BF)
        vec = jnp.concatenate([norm_gain, b_up, b_down]).reshape(1, -1)
        act = norm_up(resid, vec, w_up)
        return settle(down_scatter(act, w_down, resid, vec, tok))

    return jax.shard_map(local_block, mesh=mesh, in_specs=(tok_spec, P(), P(), P(), P(), P(), P(), P()), out_specs=tok_spec, check_vma=False)
```

```python
import functools
import math

import jax
import jax.numpy as jnp
from jax import lax
from jax.experimental import pallas as pl
from jax.experimental.pallas import tpu as pltpu
from jax.sharding import PartitionSpec as P

NORM_EPS = 1e-6
VMEM_BYTES = 63 * 2**20
BF = jnp.bfloat16
F32 = jnp.float32
ANY = pl.BlockSpec(memory_space=pl.ANY)

ORDER = (0, 2, 4, 1, 6, 3, 5, 7)
PIECES = 8


def peer(rel):
    i, j = lax.axis_index("cp"), lax.axis_index("sp")
    kx, kc, ky = rel // 4, (rel // 2) % 2, rel % 2
    x = lax.rem(i // 2 + kx, 2)
    core = lax.rem(lax.rem(i, 2) + kc, 2)
    cp, sp = x * 2 + core, lax.rem(j + ky, 2)
    return {"cp": cp, "sp": sp}, cp * 2 + sp


def arrive():
    bar = pltpu.get_barrier_semaphore()
    for rel in range(1, PIECES):
        pl.semaphore_signal(bar, inc=1, device_id=peer(rel)[0], device_id_type=pl.DeviceIdType.MESH)


def await_all():
    pl.semaphore_wait(pltpu.get_barrier_semaphore(), PIECES - 1)


def params(**kw):
    return pltpu.CompilerParams(vmem_limit_bytes=VMEM_BYTES, **kw)


def qkv_kernel(hid, w_hbm, o_ref, row_out, xs, wbuf, w_sem, own_sem, send_sem, recv_sem, out_sem, *, n_tiles, kp, group):
    t = pl.program_id(0)
    last = pl.num_programs(0) - 1
    chunk = t // n_tiles
    dim, hb, hd = wbuf.shape[1:]
    per = n_tiles // w_hbm.shape[1]

    def weights(step):
        tile = lax.rem(step, n_tiles)
        heads = pl.ds(pl.multiple_of(lax.rem(tile, per) * hb, hb), hb)
        return pltpu.make_async_copy(w_hbm.at[:, tile // per, heads], wbuf.at[lax.rem(step, 2)], w_sem.at[lax.rem(step, 2)])

    def send(slot):
        dev, row = peer(ORDER[slot])
        return pltpu.make_async_remote_copy(
            src_ref=hid.at[row], dst_ref=xs.at[slot], send_sem=send_sem.at[slot - 1], recv_sem=recv_sem.at[slot - 1],
            device_id=dev, device_id_type=pl.DeviceIdType.MESH)

    def keep(slot):
        return pltpu.make_async_copy(xs.at[slot], row_out.at[slot], out_sem.at[slot])

    @pl.when(t == 0)
    def _():
        own = pltpu.make_async_copy(hid.at[peer(0)[1]], xs.at[0], own_sem)
        own.start()
        weights(t).start()
        arrive()
        await_all()
        for slot in range(1, PIECES):
            send(slot).start()
        own.wait()
        keep(0).start()

    for c in range(PIECES // 2):
        @pl.when(t == c * n_tiles)
        def _(c=c):
            for slot in (2 * c, 2 * c + 1):
                if slot:
                    send(slot).wait_recv()
                    keep(slot).start()

    @pl.when(t < last)
    def _():
        weights(t + 1).start()

    weights(t).wait()

    w_ref = wbuf.at[lax.rem(t, 2)]
    for h in range(0, hb, group):
        acc = None
        for k in range(0, dim, kp):
            turned = jnp.swapaxes(w_ref[k:k + kp, h:h + group], 0, 1)
            cols = jnp.concatenate([turned[g] for g in range(group)], axis=1)
            x = xs[pl.ds(2 * chunk, 2), :, k:k + kp]
            d = jnp.dot(x.reshape(-1, kp), cols, preferred_element_type=F32)
            acc = d if acc is None else acc + d
        o_ref[:, h * hd:(h + group) * hd] = acc.astype(BF)

    @pl.when(t == last)
    def _():
        for slot in range(PIECES):
            if slot:
                send(slot).wait_send()
            keep(slot).wait()


def gather_qkv(hidden, w, hb=16):
    pieces, tok, dim = hidden.shape
    _, kinds, heads, head_dim = w.shape
    per, width, tn = heads // hb, kinds * heads * head_dim, hb * head_dim
    n_tiles = kinds * per
    return pl.pallas_call(
        functools.partial(qkv_kernel, n_tiles=n_tiles, kp=256, group=8), name="gather_qkv", grid=(pieces // 2 * n_tiles,),
        in_specs=[ANY, ANY],
        out_specs=[pl.BlockSpec((2 * tok, tn), lambda t: (t // n_tiles, t % n_tiles)), ANY],
        out_shape=[jax.ShapeDtypeStruct((pieces * tok, width), BF), jax.ShapeDtypeStruct(hidden.shape, BF)],
        scratch_shapes=[pltpu.VMEM(hidden.shape, BF), pltpu.VMEM((2, dim, hb, head_dim), BF), pltpu.SemaphoreType.DMA((2,)),
                        pltpu.SemaphoreType.DMA, pltpu.SemaphoreType.DMA((pieces - 1,)),
                        pltpu.SemaphoreType.DMA((pieces - 1,)), pltpu.SemaphoreType.DMA((pieces,))],
        compiler_params=params(collective_id=0, has_side_effects=True))(hidden, w)


def attn_kernel(q_ref, k_ref, v_ref, qn_ref, kn_ref, o_ref, ve_ref, sc_ref, *, bq, hd, dim):
    tok = q_ref.shape[0]
    n = tok // bq
    coef = dim ** -0.5 * math.log2(math.e)

    def dot_nt(a, b):
        return lax.dot_general(a, b, (((1,), (1,)), ((), ())), preferred_element_type=F32)

    @pl.when(pl.program_id(0) == 0)
    def _():
        ve_ref[:, dim:] = jnp.zeros((tok, dim), BF)
        sc_ref[...] = dot_nt(q_ref[:bq, :dim], k_ref[:, :dim])

    def scores(g):
        h, i = divmod(g, n)
        if h < hd:
            return dot_nt(q_ref[i * bq:(i + 1) * bq, h * dim:(h + 1) * dim], k_ref[:, h * dim:(h + 1) * dim])
        return dot_nt(qn_ref[...], kn_ref[...])

    s = sc_ref[...]
    for g in range(n * hd):
        h, i = divmod(g, n)
        if i == 0:
            ve_ref[:, :dim] = v_ref[:, h * dim:(h + 1) * dim]
        ahead = scores(g + 1)
        m = jnp.max(s, axis=-1, keepdims=True)
        p = jnp.exp2((s - m) * coef)
        total = jnp.sum(p, axis=-1, keepdims=True)
        o = jnp.dot(p.astype(BF), ve_ref[...], preferred_element_type=F32)
        o_ref[i * bq:(i + 1) * bq, h * dim:(h + 1) * dim] = (o[:, :dim] * (1.0 / total)).astype(BF)
        s = ahead
    sc_ref[...] = s


def attention(qkv, heads, dim, bq=256, hd=4):
    tok = qkv.shape[0]
    steps = heads // hd
    cols = lambda j: pl.BlockSpec((tok, hd * dim), lambda t: (0, j * steps + t))
    ahead = lambda t: jnp.minimum((t + 1) * hd, heads - 1)
    return pl.pallas_call(
        functools.partial(attn_kernel, bq=bq, hd=hd, dim=dim), name="attention", grid=(steps,),
        in_specs=[cols(0), cols(1), cols(2), pl.BlockSpec((bq, dim), lambda t: (0, ahead(t))),
                  pl.BlockSpec((tok, dim), lambda t: (0, heads + ahead(t)))],
        out_specs=pl.BlockSpec((tok, hd * dim), lambda t: (0, t)),
        out_shape=jax.ShapeDtypeStruct((tok, heads * dim), BF),
        scratch_shapes=[pltpu.VMEM((tok, 2 * dim), BF), pltpu.VMEM((bq, tok), F32)],
        compiler_params=params())(*[qkv] * 5)


TANH_LIN = math.sqrt(2 / math.pi)
TANH_CUB = TANH_LIN * 0.044715


def gelu(z):
    half = 0.5 * z
    return half + half * jnp.tanh(z * (TANH_LIN + TANH_CUB * (z * z)))


def up_kernel(r_hbm, v_ref, w_hbm, o_ref, xn, rbuf, z0, z1, wbuf, w_sem, sem, *, tm, tn, sub, kp, ep, rn):
    t = pl.program_id(0)
    tok, dim = xn.shape
    nm, last = tok // tm, pl.num_programs(0) - 1
    rc = rbuf.shape[1]

    def weights(n):
        cols = pl.ds(pl.multiple_of(n * tn, tn), tn)
        return pltpu.make_async_copy(w_hbm.at[:, cols], wbuf.at[lax.rem(n, 2)], w_sem.at[lax.rem(n, 2)])

    @pl.when(t == 0)
    def _():
        fetch = lambda i: pltpu.make_async_copy(r_hbm.at[pl.ds(i * rc, rc)], rbuf.at[lax.rem(i, 2)], sem.at[lax.rem(i, 2)])
        fetch(0).start()
        weights(0).start()
        gain = v_ref[:, :dim].astype(F32)

        def block(i, _):
            @pl.when(i + 1 < tok // rc)
            def _():
                fetch(i + 1).start()

            fetch(i).wait()

            def rows(u, _):
                at = pl.multiple_of(u * rn, rn)
                x = rbuf[lax.rem(i, 2), pl.ds(at, rn), :].astype(F32)
                inv = lax.rsqrt(jnp.mean(x * x, axis=-1, keepdims=True) + NORM_EPS)
                xn[pl.ds(pl.multiple_of(i * rc + at, rn), rn), :] = (x * inv * gain).astype(BF)
                return 0

            return lax.fori_loop(0, rc // rn, rows, 0)

        lax.fori_loop(0, tok // rc, block, 0)

    n = t // nm

    @pl.when((t < last) & (lax.rem(t, nm) == 0))
    def _():
        @pl.when(t + nm < last)
        def _():
            weights(n + 1).start()

        weights(n).wait()

    w_ref = wbuf.at[lax.rem(n, 2)]
    col = jnp.maximum((t - 1) // nm, 0) * tn
    bias = lambda: v_ref[:, pl.ds(pl.multiple_of(dim + col, tn), tn)].astype(F32)

    def tile(z_now, z_prev):
        base = pl.multiple_of(lax.rem(t, nm) * tm, tm)
        b = bias()
        parts = [(e, c) for e in range(0, tm, ep) for c in range(0, tn, sub)]
        share = len(parts) / (tm // sub * (tn // sub) * (dim // kp))
        done = step = 0
        for c in range(0, tn, sub):
            for r in range(0, tm, sub):
                acc = None
                for k in range(0, dim, kp):
                    d = jnp.dot(xn[pl.ds(base + r, sub), k:k + kp], w_ref[k:k + kp, c:c + sub], preferred_element_type=F32)
                    acc = d if acc is None else acc + d
                    step += 1
                    while done < step * share - 1e-9:
                        e, ec = parts[done]
                        done += 1
                        o_ref[e:e + ep, ec:ec + sub] = gelu(z_prev[e:e + ep, ec:ec + sub] + b[:, ec:ec + sub]).astype(BF)
                z_now[r:r + sub, c:c + sub] = acc

    for par, (za, zb) in enumerate(((z0, z1), (z1, z0))):
        @pl.when((t < last) & (lax.rem(t, 2) == par))
        def _(za=za, zb=zb):
            tile(za, zb)

    @pl.when(t == last)
    def _():
        def rows(i, _):
            at = pl.ds(pl.multiple_of(i * 64, 64), 64)
            o_ref[at, :] = gelu(z1[at, :] + bias()).astype(BF)
            return 0

        lax.fori_loop(0, tm // 64, rows, 0)


def norm_up(resid, vec, w, tm=1024, tn=1024):
    tok, dim = resid.shape
    nm = tok // tm
    tiles = nm * (w.shape[1] // tn)
    prev = lambda t: jnp.maximum(t - 1, 0)
    return pl.pallas_call(
        functools.partial(up_kernel, tm=tm, tn=tn, sub=512, kp=256, ep=32, rn=128), name="norm_up", grid=(tiles + 1,),
        in_specs=[ANY, pl.BlockSpec(vec.shape, lambda t: (0, 0)), ANY],
        out_specs=pl.BlockSpec((tm, tn), lambda t: (prev(t) % nm, prev(t) // nm)),
        out_shape=jax.ShapeDtypeStruct((tok, w.shape[1]), BF),
        scratch_shapes=[pltpu.VMEM((tok, dim), BF), pltpu.VMEM((2, 256, dim), BF), pltpu.VMEM((tm, tn), F32),
                        pltpu.VMEM((tm, tn), F32), pltpu.VMEM((2, dim, tn), BF), pltpu.SemaphoreType.DMA((2,)),
                        pltpu.SemaphoreType.DMA((2,))],
        compiler_params=params())(resid, vec, w)


SLOTS = 3


def down_kernel(a_ref, w_ref, r_ref, b_ref, out, acc, obuf, own_sem, send_sem, recv_sem, *, tn, nk, nn):
    t = pl.program_id(0)
    tiles = PIECES // 2 * nn
    q, k = t // nk, lax.rem(t, nk)
    tok = out.shape[1]

    def moves(tile):
        chunk = PIECES // 2 - 1 - tile // nn
        cols = pl.ds(tile % nn * tn, tn)
        my_row = peer(0)[1]
        for p in range(2):
            slot = 2 * chunk + p
            src = obuf.at[tile % SLOTS, pl.ds(p * tok, tok)]
            dst = out.at[my_row, :, cols]
            if slot == 0:
                yield pltpu.make_async_copy(src, dst, own_sem.at[tile % nn]), None
            else:
                yield None, pltpu.make_async_remote_copy(
                    src_ref=src, dst_ref=dst, send_sem=send_sem.at[tile, p], recv_sem=recv_sem.at[tile % nn, slot - 1],
                    device_id=peer(ORDER[slot])[0], device_id_type=pl.DeviceIdType.MESH)

    def sent(tile):
        for local, remote in moves(tile):
            if remote:
                remote.wait_send()
            else:
                local.wait()

    @pl.when(t == 0)
    def _():
        arrive()

    @pl.when(t == nk)
    def _():
        await_all()

    for tile in range(tiles):
        @pl.when(t == (tile + 1) * nk)
        def _(tile=tile):
            for local, remote in moves(tile):
                (local or remote).start()

        if tile + SLOTS < tiles:
            @pl.when(t == (tile + SLOTS) * nk + nk - 1)
            def _(tile=tile):
                sent(tile)

    @pl.when(q < tiles)
    def _():
        @pl.when(k < nk - 1)
        def _():
            d = jnp.dot(a_ref[...], w_ref[...], preferred_element_type=F32)
            acc[...] = jnp.where(k == 0, d, acc[...] + d)

        @pl.when(k == nk - 1)
        def _():
            d = jnp.dot(a_ref[...], w_ref[...], preferred_element_type=F32)
            y = r_ref[...].astype(F32) + ((acc[...] + d) + b_ref[...].astype(F32))
            obuf[lax.rem(q, SLOTS)] = y.astype(BF)

    @pl.when(q == tiles)
    def _():
        for tile in range(tiles - SLOTS, tiles):
            sent(tile)
        for tile in range(tiles):
            for _, remote in moves(tile):
                if remote:
                    remote.wait_recv()


def down_scatter(act, w, resid, b, tok, tn=2048, tk=4096):
    rows, kdim = act.shape
    dim = w.shape[1]
    tm, nn, nk = 2 * tok, dim // tn, kdim // tk
    tiles = PIECES // 2 * nn
    cur = lambda t: jnp.minimum(t, tiles * nk - 1)
    m_of = lambda t: PIECES // 2 - 1 - cur(t) // (nk * nn)
    n_of = lambda t: (cur(t) // nk) % nn
    return pl.pallas_call(
        functools.partial(down_kernel, tn=tn, nk=nk, nn=nn), name="down_scatter", grid=(tiles * nk + 1,),
        in_specs=[pl.BlockSpec((tm, tk), lambda t: (m_of(t), cur(t) % nk)),
                  pl.BlockSpec((tk, tn), lambda t: (cur(t) % nk, n_of(t))),
                  pl.BlockSpec((tm, tn), lambda t: (m_of(t), n_of(t))),
                  pl.BlockSpec((1, tn), lambda t: (0, b.shape[1] // tn - nn + n_of(t)))],
        out_specs=ANY, out_shape=jax.ShapeDtypeStruct((PIECES, tok, dim), BF),
        scratch_shapes=[pltpu.VMEM((tm, tn), F32), pltpu.VMEM((SLOTS, tm, tn), BF), pltpu.SemaphoreType.DMA((nn,)),
                        pltpu.SemaphoreType.DMA((tiles, 2)), pltpu.SemaphoreType.DMA((nn, PIECES - 1))],
        compiler_params=params(collective_id=1, has_side_effects=True))(act, w, resid, b)


def settle_kernel(x, out, buf, in_sem, out_sem):
    load = [pltpu.make_async_copy(x.at[i], buf.at[i], in_sem.at[i]) for i in range(PIECES)]
    save = [pltpu.make_async_copy(buf.at[i], out.at[i], out_sem.at[i]) for i in range(PIECES)]
    for c in load:
        c.start()
    for a, b in zip(load, save):
        a.wait()
        b.start()
    for c in save:
        c.wait()


def settle(x):
    return pl.pallas_call(
        settle_kernel, name="settle", in_specs=[ANY], out_specs=ANY, out_shape=jax.ShapeDtypeStruct(x.shape, x.dtype),
        scratch_shapes=[pltpu.VMEM(x.shape, x.dtype), pltpu.SemaphoreType.DMA((PIECES,)), pltpu.SemaphoreType.DMA((PIECES,))],
        compiler_params=params())(x)


def solution(mesh):
    tok_spec = P("dp", ("cp", "sp"), None)

    def local_block(hidden, w_qkv, w_out, norm_gain, w_up, b_up, w_down, b_down):
        pieces, tok, dim = hidden.shape
        _, _, heads, head_dim = w_qkv.shape
        qkv, row = gather_qkv(hidden, w_qkv)
        attn = attention(qkv, heads, head_dim)
        attn_out = jnp.dot(attn, w_out.reshape(heads * head_dim, dim), preferred_element_type=F32).astype(BF)
        resid = (row.reshape(pieces * tok, dim).astype(F32) + attn_out.astype(F32)).astype(BF)
        vec = jnp.concatenate([norm_gain, b_up, b_down]).reshape(1, -1)
        act = norm_up(resid, vec, w_up)
        return settle(down_scatter(act, w_down, resid, vec, tok))

    return jax.shard_map(local_block, mesh=mesh, in_specs=(tok_spec, P(), P(), P(), P(), P(), P(), P()), out_specs=tok_spec, check_vma=False)
```
